128 devices in a mesh: fsdp: 16 (over z, x_lo, core), cols: 8 (over y, x_hi).
Axes of the slice: x: 4 (x_hi: 2, x_lo: 2; x = x_hi * 2 + x_lo), y: 4, z: 4, core: 2. Of those that a mesh axis runs over, the one named last changes fastest.
Arguments:
- weight_query: bfloat16 [5120, 5120], P('fsdp', 'cols'), may hold values from -0.078125 to 0.078125
- low_query: bfloat16 [5120, 32], P('fsdp'), may hold values from -0.078125 to 0.078125
- high_query: bfloat16 [32, 5120], P(None, 'cols'), may hold values from -1 to 1
- weight_key: bfloat16 [5120, 5120], P('fsdp', 'cols'), may hold values from -0.078125 to 0.078125
- low_key: bfloat16 [5120, 32], P('fsdp'), may hold values from -0.078125 to 0.078125
- high_key: bfloat16 [32, 5120], P(None, 'cols'), may hold values from -1 to 1
- weight_value: bfloat16 [5120, 5120], P('fsdp', 'cols'), may hold values from -0.078125 to 0.078125
- low_value: bfloat16 [5120, 32], P('fsdp'), may hold values from -0.078125 to 0.078125
- high_value: bfloat16 [32, 5120], P(None, 'cols'), may hold values from -1 to 1
- weight_mixed: bfloat16 [5120, 5120], P('cols', 'fsdp'), may hold values from -0.078125 to 0.078125
- low_mixed: bfloat16 [5120, 32], P('cols'), may hold values from -0.078125 to 0.078125
- high_mixed: bfloat16 [32, 5120], P(None, 'fsdp'), may hold values from -1 to 1
- norm_train: float32 [5120], P(('fsdp', 'cols')), may hold values from 0.25 to 1.75
- norm_step: float32 [5120], P(('fsdp', 'cols')), may hold values from -0.3 to 0.3
Outputs:
- ready_query: bfloat16 [5120, 5120], P(None, 'cols')
- ready_key: bfloat16 [5120, 5120], P(None, 'cols')
- ready_value: bfloat16 [5120, 5120], P(None, 'cols')
- ready_mixed: bfloat16 [5120, 5120], P('cols')
- serve_norm: bfloat16 [5120], replicated
The draws below stay inside these ranges and needn't reach their ends.
All inputs are finite; a program needn't handle non-finite values.
Results may differ from the reference program's by a relative error of at most 0.001.
Values may be sent and summed in bfloat16 or wider, within the bound.
A program may use at most 192 MiB of HBM per device.

```python
import jax
import jax.numpy as jnp

D_MODEL = 5120
Q_DIM = 5120
KV_DIM = 5120
RANK = 32


def block_levels(stream_key, extent, pieces, smallest, high):
    level, own = 1.0, jax.random.fold_in(stream_key, 6)
    for dim, shards_of in pieces:
        steps = jnp.exp(jax.random.uniform(jax.random.fold_in(own, dim), (shards_of,), jnp.float32, smallest / len(pieces), high / len(pieces)))
        level = level * jnp.repeat(steps, extent[dim] // shards_of).reshape([-1 if axis == dim else 1 for axis in range(len(extent))])
    return level


def gaussian(stream_key, extent, deviation, limit, split=(), dtype=jnp.bfloat16):
    values = deviation * jax.random.normal(stream_key, extent, jnp.float32)
    if split:
        values = values * block_levels(stream_key, extent, split, -0.22, 0.18)
    return jnp.clip(values, -limit, limit).astype(dtype)


def setup_inputs(seed: int = 0) -> dict:
    arg_keys = jax.random.split(jax.random.key(seed), 15)
    weight_query = gaussian(arg_keys[0], (D_MODEL, Q_DIM), D_MODEL ** -0.5, 0.078125, ((0, 16), (1, 8)))
    low_query = gaussian(arg_keys[1], (D_MODEL, RANK), D_MODEL ** -0.5, 0.078125, ((0, 16),))
    high_query = gaussian(arg_keys[2], (RANK, Q_DIM), RANK ** -0.5, 1.0, ((1, 8),))
    weight_key = gaussian(arg_keys[3], (D_MODEL, KV_DIM), D_MODEL ** -0.5, 0.078125, ((0, 16), (1, 8)))
    low_key = gaussian(arg_keys[4], (D_MODEL, RANK), D_MODEL ** -0.5, 0.078125, ((0, 16),))
    high_key = gaussian(arg_keys[5], (RANK, KV_DIM), RANK ** -0.5, 1.0, ((1, 8),))
    weight_value = gaussian(arg_keys[6], (D_MODEL, KV_DIM), D_MODEL ** -0.5, 0.078125, ((0, 16), (1, 8)))
    low_value = gaussian(arg_keys[7], (D_MODEL, RANK), D_MODEL ** -0.5, 0.078125, ((0, 16),))
    high_value = gaussian(arg_keys[8], (RANK, KV_DIM), RANK ** -0.5, 1.0, ((1, 8),))
    weight_mixed = gaussian(arg_keys[9], (Q_DIM, D_MODEL), Q_DIM ** -0.5, 0.078125, ((0, 8), (1, 16)))
    low_mixed = gaussian(arg_keys[10], (Q_DIM, RANK), Q_DIM ** -0.5, 0.078125, ((0, 8),))
    high_mixed = gaussian(arg_keys[11], (RANK, D_MODEL), RANK ** -0.5, 1.0, ((1, 16),))
    norm_train = jnp.clip(1.0 + 0.15 * jax.random.normal(arg_keys[12], (D_MODEL,), jnp.float32), 0.25, 1.75)
    norm_step = jnp.clip(jax.random.uniform(arg_keys[13], (D_MODEL,), jnp.float32, -0.3, 0.3) * block_levels(arg_keys[13], (D_MODEL,), ((0, 128),), -0.4, 0.0), -0.3, 0.3)
    return dict(weight_query=weight_query, low_query=low_query, high_query=high_query, weight_key=weight_key, low_key=low_key, high_key=high_key, weight_value=weight_value, low_value=low_value, high_value=high_value, weight_mixed=weight_mixed, low_mixed=low_mixed, high_mixed=high_mixed, norm_train=norm_train, norm_step=norm_step)


mix_rate = 2.0


def reference(weight_query, low_query, high_query, weight_key, low_key, high_key, weight_value, low_value, high_value, weight_mixed, low_mixed, high_mixed, norm_train, norm_step):
    latest_query = weight_query.astype(jnp.float32) + mix_rate * jnp.dot(low_query, high_query, preferred_element_type=jnp.float32)
    latest_key = weight_key.astype(jnp.float32) + mix_rate * jnp.dot(low_key, high_key, preferred_element_type=jnp.float32)
    latest_value = weight_value.astype(jnp.float32) + mix_rate * jnp.dot(low_value, high_value, preferred_element_type=jnp.float32)
    latest_mixed = weight_mixed.astype(jnp.float32) + mix_rate * jnp.dot(low_mixed, high_mixed, preferred_element_type=jnp.float32)
    ready_query = latest_query.astype(jnp.bfloat16)
    ready_key = latest_key.astype(jnp.bfloat16)
    ready_value = latest_value.astype(jnp.bfloat16)
    ready_mixed = latest_mixed.astype(jnp.bfloat16)
    serve_norm = (norm_train + norm_step).astype(jnp.bfloat16)
    return ready_query, ready_key, ready_value, ready_mixed, serve_norm
```

```python
import functools
import heapq

import jax
import jax.numpy as jnp
from jax import lax
from jax.experimental import pallas as pl
from jax.experimental.pallas import tpu as pltpu
from jax.sharding import PartitionSpec as P

mix_rate = 2.0

Z, X, CORES = 4, 2, 2
CHIPS = Z * X
ROWS, WIDTH, RANK = 320, 640, 32
FULL = ROWS * CHIPS * CORES
RING_FIRST, ACROSS_FIRST = 0, 1
PART = ((0, 144), (144, 176))
RIGHT, LEFT, ACROSS = 0, 1, 2
LINKS = (RIGHT, LEFT, ACROSS)


def onward(dz, dx, array, part, via):
    links = []
    if part == RING_FIRST and dx == 0:
        links.append(ACROSS)
    if part == ACROSS_FIRST and (dz, dx) == (0, 1):
        links += [RIGHT, LEFT]
    if via == RIGHT and dz == 3 and array < 2:
        links.append(RIGHT)
    if via == LEFT and dz == 1 and array >= 2:
        links.append(LEFT)
    return links


def seen_by_receiver(dz, dx, link):
    if link == RIGHT:
        return (dz - 1) % Z, dx
    if link == LEFT:
        return (dz + 1) % Z, dx
    return dz, 1 - dx


def first_sends():
    early, late = [], []
    for array in range(4):
        into = early if array < 3 else late
        into += [(ACROSS, array, ACROSS_FIRST), (RIGHT, array, RING_FIRST), (LEFT, array, RING_FIRST)]
    for array in range(4):
        late += [(ACROSS, array, RING_FIRST), (RIGHT, array, ACROSS_FIRST), (LEFT, array, ACROSS_FIRST)]
    return early, late


def arrivals():
    rate, latency = 46.7e3, 2.0
    free = [0.0] * 3
    queue, order = [], []

    def send(now, link, unit):
        took = PART[unit[3]][1] * WIDTH * 2 / rate
        free[link] = max(free[link], now) + took
        heapq.heappush(queue, (free[link] + latency, len(queue) + 1000 * len(order), link, unit))

    early, late = first_sends()
    for link, array, part in early + late:
        send(0.0, link, (0, 0, array, part))
    while queue:
        now, _, via, (dz, dx, array, part) = heapq.heappop(queue)
        dz, dx = seen_by_receiver(dz, dx, via)
        order.append((dz, dx, array, part, via))
        for link in onward(dz, dx, array, part, via):
            send(now, link, (dz, dx, array, part))
    return order


def merge(weight, left, right):
    product = lax.dot_general(left, right, (((0,), (0,)), ((), ())), preferred_element_type=jnp.float32)
    return (weight.astype(jnp.float32) + mix_rate * product).astype(jnp.bfloat16)


def gather_kernel(
    cols,
    weight_query, low_query, high_query,
    weight_key, low_key, high_key,
    weight_value, low_value, high_value,
    weight_mixed, low_mixed, high_mixed,
    norm_train, norm_step,
    full_query, full_key, full_value, full_mixed, norm_slots,
    weights, lefts, rights, mixed_pair, norms, norm_parts,
    in_sem, link_send, link_recv, core_send, core_recv, pair_sem, norm_send, near_recv, far_recv,
):
    f, c = lax.axis_index("fsdp"), lax.axis_index("cols")
    z, x, core = lax.div(f, X * CORES), lax.rem(lax.div(f, CORES), X), lax.rem(f, CORES)
    chip = lax.div(f, CORES)
    fulls = (full_query, full_key, full_value, full_mixed)

    def at(device_z, device_x, device_core):
        return device_z * (X * CORES) + device_x * CORES + device_core

    neighbour = {
        RIGHT: at(lax.rem(z + 1, Z), x, core),
        LEFT: at(lax.rem(z + Z - 1, Z), x, core),
        ACROSS: at(z, 1 - x, core),
    }
    twin = at(z, x, 1 - core)

    loads = []

    def load(source, target):
        copy = pltpu.make_async_copy(source, target, in_sem.at[len(loads)])
        copy.start()
        loads.append(copy)

    inputs = (
        (weight_query, low_query, high_query),
        (weight_key, low_key, high_key),
        (weight_value, low_value, high_value),
        (weight_mixed, high_mixed, low_mixed),
    )
    for k, (weight, left, right) in enumerate(inputs):
        load(weight, weights.at[k])
        load(left, lefts.at[k])
        load(right, rights.at[k])
    load(norm_train, norms.at[0])
    load(norm_step, norms.at[1])

    near = [(dc, dk) for dc in range(cols) for dk in range(CORES) if (dc, dk) != (0, 0)]
    far = [(dz, dx) for dz in range(Z) for dx in range(X) if (dz, dx) != (0, 0)]

    def near_id(dc, dk):
        return {"fsdp": at(z, x, lax.rem(core + dk, CORES)), "cols": lax.rem(c + dc, cols)}

    def far_id(dz, dx):
        return {"fsdp": at(lax.rem(z + dz, Z), lax.rem(x + dx, X), core)}

    barrier = pltpu.get_barrier_semaphore()
    for peer in [near_id(*d) for d in near] + [far_id(*d) for d in far]:
        pl.semaphore_signal(barrier, inc=1, device_id=peer, device_id_type=pl.DeviceIdType.MESH)

    def wait_loads(k):
        for copy in loads[3 * k : 3 * k + 3]:
            copy.wait()

    own_rows = pl.ds(pl.multiple_of(f * ROWS, 16), ROWS)
    wait_loads(3)
    own_half = pl.ds(pl.multiple_of(core * ROWS, 16), ROWS)
    mixed_pair[own_half, :] = merge(weights[3], lefts[3], rights[3])
    for k in range(3):
        wait_loads(k)
        fulls[k][own_rows, :] = merge(weights[k], lefts[k], rights[k])
    pl.semaphore_wait(barrier, len(near) + len(far))

    sends = []

    def remote(source, target, send_sem, recv_sem, device):
        copy = pltpu.make_async_remote_copy(
            src_ref=source,
            dst_ref=target,
            send_sem=send_sem,
            recv_sem=recv_sem,
            device_id=device if isinstance(device, dict) else {"fsdp": device},
            device_id_type=pl.DeviceIdType.MESH,
        )
        copy.start()
        sends.append(copy)

    def view(dz, dx, device_core, array, start, rows):
        block = lax.rem(z + dz, Z) * X + lax.rem(x + dx, X)
        if array < 3:
            first = (block * CORES + device_core) * ROWS + start
            return fulls[array].at[pl.ds(pl.multiple_of(first, 16), rows), :]
        first = device_core * ROWS + start
        return full_mixed.at[
            pl.ds(pl.multiple_of(first, 16), rows), pl.ds(pl.multiple_of(block * WIDTH, 128), WIDTH)
        ]

    def place(dz, dx, array, part):
        return ((dz * X + dx) * 4 + array) * 2 + part

    counts = {"link": 0, "core": 0}

    def send_on(link, dz, dx, array, part):
        block = view(dz, dx, core, array, *PART[part])
        there = place(*seen_by_receiver(dz, dx, link), array, part)
        remote(block, block, link_send.at[counts["link"]], link_recv.at[there], neighbour[link])
        counts["link"] += 1

    def hand_over(dz, dx, array, part):
        block = view(dz, dx, core, array, *PART[part])
        remote(block, block, core_send.at[counts["core"]], core_recv.at[place(dz, dx, array, part)], twin)
        counts["core"] += 1

    early, late = first_sends()
    half = mixed_pair.at[own_half, :]
    remote(half, half, pair_sem.at[0], pair_sem.at[1], twin)
    pair = sends[-1]
    for link, array, part in early:
        send_on(link, 0, 0, array, part)
    for array in range(3):
        for part in (RING_FIRST, ACROSS_FIRST):
            hand_over(0, 0, array, part)

    for copy in loads[12:]:
        copy.wait()
    piece = norms.shape[-1]
    gain = (norms[0] + norms[1]).astype(jnp.bfloat16)
    gain = jnp.broadcast_to(gain.astype(jnp.float32), (8, piece)).astype(jnp.bfloat16)
    offset = (core * cols + c) * piece
    lane = lax.broadcasted_iota(jnp.int32, (piece, 128), 1)
    element = lax.broadcasted_iota(jnp.int32, (piece, 128), 0)
    row = lax.broadcasted_iota(jnp.int32, (8, 128), 0)
    tile = jnp.zeros((8, 128), jnp.float32)
    for r in range(5):
        hot = jnp.where(lane + 128 * r == element + offset, 1.0, 0.0).astype(jnp.bfloat16)
        spread = jnp.dot(gain, hot, preferred_element_type=jnp.float32)
        tile = jnp.where(row == r, spread, tile)
    norm_parts[0] = tile

    pair.wait_recv()
    turned = mixed_pair[...].astype(jnp.float32).T.astype(jnp.bfloat16)
    full_mixed[:, pl.ds(pl.multiple_of(chip * WIDTH, 128), WIDTH)] = turned

    for n, (dc, dk) in enumerate(near):
        slot = ((cols - dc) % cols) * CORES + dk
        remote(norm_parts.at[0], norm_parts.at[slot], norm_send.at[n], near_recv.at[slot], near_id(dc, dk))

    for link, array, part in late:
        send_on(link, 0, 0, array, part)

    def sum_norms():
        total = norm_parts[0]
        for slot in range(1, cols * CORES):
            pltpu.make_async_copy(norm_parts.at[0], norm_parts.at[slot], near_recv.at[slot]).wait()
            total = total + norm_parts[slot]
        norm_slots[chip] = total

    def spread_norms():
        for n, (dz, dx) in enumerate(far):
            slot = (-dz % Z) * X + dx
            remote(
                norm_slots.at[chip], norm_slots.at[chip], norm_send.at[len(near) + n], far_recv.at[slot], far_id(dz, dx)
            )

    def came_in(sem, dz, dx, device_core, array, part):
        block = view(dz, dx, device_core, array, *PART[part])
        pltpu.make_async_copy(block, block, sem.at[place(dz, dx, array, part)]).wait()

    for n, (dz, dx, array, part, via) in enumerate(arrivals()):
        came_in(link_recv, dz, dx, core, array, part)
        for link in onward(dz, dx, array, part, via):
            send_on(link, dz, dx, array, part)
        hand_over(dz, dx, array, part)
        if n == 10:
            sum_norms()
        if n == 12:
            spread_norms()

    for dz, dx in far:
        slot = dz * X + dx
        there = lax.rem(z + dz, Z) * X + lax.rem(x + dx, X)
        pltpu.make_async_copy(norm_slots.at[there], norm_slots.at[there], far_recv.at[slot]).wait()
    for dz in range(Z):
        for dx in range(X):
            for array in range(4):
                for part in (RING_FIRST, ACROSS_FIRST):
                    if (dz, dx) != (0, 0) or array < 3:
                        came_in(core_recv, dz, dx, 1 - core, array, part)
    for copy in sends:
        copy.wait_send()


def store_kernel(query, key, value, mixed, slots, out_query, out_key, out_value, out_mixed, out_norm, sems):
    copies = []
    for source, target in ((query, out_query), (key, out_key), (value, out_value), (mixed, out_mixed)):
        rows = source.shape[0] // 4
        for k in range(4):
            part = pl.ds(k * rows, rows)
            copy = pltpu.make_async_copy(source.at[part, :], target.at[part, :], sems.at[len(copies)])
            copy.start()
            copies.append(copy)
    gains = jnp.concatenate([slots[k][:5] for k in range(CHIPS)], axis=0)
    out_norm[...] = gains.astype(jnp.bfloat16)
    for copy in copies:
        copy.wait()


def per_device(
    cols,
    weight_query, low_query, high_query,
    weight_key, low_key, high_key,
    weight_value, low_value, high_value,
    weight_mixed, low_mixed, high_mixed,
    norm_train, norm_step,
):
    tall, wide = (FULL, WIDTH), (WIDTH, FULL)
    piece = norm_train.shape[0]
    anywhere = pl.BlockSpec(memory_space=pl.ANY)
    in_vmem = pl.BlockSpec(memory_space=pltpu.VMEM)
    n_link = sum(len(onward(*u)) for u in arrivals()) + sum(len(s) for s in first_sends())
    n_core = len(arrivals()) + 6
    fulls = pl.pallas_call(
        functools.partial(gather_kernel, cols),
        name="gather",
        out_shape=[pltpu.VMEM(tall, jnp.bfloat16)] * 3
        + [pltpu.VMEM(wide, jnp.bfloat16), pltpu.VMEM((CHIPS, 8, 128), jnp.float32)],
        in_specs=[pl.BlockSpec(memory_space=pltpu.HBM)] * 14,
        out_specs=[in_vmem] * 5,
        scratch_shapes=[
            pltpu.VMEM((4, ROWS, WIDTH), jnp.bfloat16),
            pltpu.VMEM((4, RANK, ROWS), jnp.bfloat16),
            pltpu.VMEM((4, RANK, WIDTH), jnp.bfloat16),
            pltpu.VMEM((WIDTH, WIDTH), jnp.bfloat16),
            pltpu.VMEM((2, 1, piece), jnp.float32),
            pltpu.VMEM((cols * CORES, 8, 128), jnp.float32),
            pltpu.SemaphoreType.DMA((14,)),
            pltpu.SemaphoreType.DMA((n_link,)),
            pltpu.SemaphoreType.DMA((64,)),
            pltpu.SemaphoreType.DMA((n_core,)),
            pltpu.SemaphoreType.DMA((64,)),
            pltpu.SemaphoreType.DMA((2,)),
            pltpu.SemaphoreType.DMA((cols * CORES - 1 + CHIPS - 1,)),
            pltpu.SemaphoreType.DMA((cols * CORES,)),
            pltpu.SemaphoreType.DMA((CHIPS,)),
        ],
        compiler_params=pltpu.CompilerParams(
            collective_id=0, has_side_effects=True, vmem_limit_bytes=40_690_000
        ),
    )(
        weight_query, low_query.T, high_query,
        weight_key, low_key.T, high_key,
        weight_value, low_value.T, high_value,
        weight_mixed.T, low_mixed.T, high_mixed,
        norm_train.reshape(1, piece), norm_step.reshape(1, piece),
    )
    *ready, gains = pl.pallas_call(
        store_kernel,
        name="store",
        out_shape=[jax.ShapeDtypeStruct(tall, jnp.bfloat16)] * 3
        + [jax.ShapeDtypeStruct(wide, jnp.bfloat16), jax.ShapeDtypeStruct((CHIPS * 5, 128), jnp.bfloat16)],
        in_specs=[in_vmem] * 5,
        out_specs=[anywhere] * 4 + [in_vmem],
        scratch_shapes=[pltpu.SemaphoreType.DMA((16,))],
        compiler_params=pltpu.CompilerParams(vmem_limit_bytes=4 * 2**20),
    )(*fulls)
    return (*ready, gains.reshape(-1))


def solution(mesh):
    in_specs = (
        P("fsdp", "cols"),
        P("fsdp", None),
        P(None, "cols"),
        P("fsdp", "cols"),
        P("fsdp", None),
        P(None, "cols"),
        P("fsdp", "cols"),
        P("fsdp", None),
        P(None, "cols"),
        P("cols", "fsdp"),
        P("cols", None),
        P(None, "fsdp"),
        P(("fsdp", "cols")),
        P(("fsdp", "cols")),
    )
    out_specs = (P(None, "cols"), P(None, "cols"), P(None, "cols"), P("cols", None), P())
    return jax.shard_map(
        functools.partial(per_device, mesh.shape["cols"]),
        mesh=mesh,
        in_specs=in_specs,
        out_specs=out_specs,
        check_vma=False,
    )
```

```python
import functools
import heapq

import jax
import jax.numpy as jnp
from jax import lax
from jax.experimental import pallas as pl
from jax.experimental.pallas import tpu as pltpu
from jax.sharding import PartitionSpec as P

mix_rate = 2.0

Z, X, CORES = 4, 2, 2
CHIPS = Z * X
ROWS, WIDTH, RANK = 320, 640, 32
FULL = ROWS * CHIPS * CORES
RING_FIRST, ACROSS_FIRST = (0, 144), (144, 176)
RIGHT, LEFT, ACROSS = 0, 1, 2
LINKS = (RIGHT, LEFT, ACROSS)
QUERY, KEY, VALUE, MIXED = 0, 1, 2, 3


def own_sends(array):
    return [
        (ACROSS, 0, 0, array, 1, ACROSS_FIRST),
        (RIGHT, 0, 0, array, 1, RING_FIRST),
        (LEFT, 0, 0, array, 1, RING_FIRST),
    ]


def own_rest():
    sends = []
    for first, n in ((QUERY, 3), (MIXED, 1)):
        sends += [(ACROSS, 0, 0, first, n, RING_FIRST)]
        sends += [(RIGHT, 0, 0, first, n, ACROSS_FIRST), (LEFT, 0, 0, first, n, ACROSS_FIRST)]
    return sends


def forwards():
    sends = []
    for dz in (3, 1):
        for first, n in ((QUERY, 3), (MIXED, 1)):
            sends.append((ACROSS, dz, 0, first, n, RING_FIRST))
    for rows in (RING_FIRST, ACROSS_FIRST):
        sends.append((RIGHT, 3, 0, QUERY, 2, rows))
        sends += [(LEFT, 1, 0, VALUE, 1, rows), (LEFT, 1, 0, MIXED, 1, rows)]
    for first, n in ((QUERY, 3), (MIXED, 1)):
        sends += [(RIGHT, 0, 1, first, n, ACROSS_FIRST), (LEFT, 0, 1, first, n, ACROSS_FIRST)]
    sends += [(ACROSS, 2, 0, QUERY, 2, RING_FIRST), (ACROSS, 2, 0, VALUE, 1, RING_FIRST)]
    sends += [(ACROSS, 2, 0, MIXED, 1, (0, 112)), (ACROSS, 2, 0, MIXED, 1, (112, 32))]
    sends += [(RIGHT, 3, 1, QUERY, 2, (144, 128)), (RIGHT, 3, 1, QUERY, 2, (272, 48))]
    sends += [(LEFT, 1, 1, VALUE, 1, ACROSS_FIRST)]
    sends += [(LEFT, 1, 1, MIXED, 1, (144, 128)), (LEFT, 1, 1, MIXED, 1, (272, 48))]
    return sends


def seen_by_receiver(dz, dx, link):
    if link == RIGHT:
        return (dz - 1) % Z, dx
    if link == LEFT:
        return (dz + 1) % Z, dx
    return dz, 1 - dx


def cover(dz, dx, first, n, rows):
    way = RING_FIRST if rows[0] < ACROSS_FIRST[0] else ACROSS_FIRST
    return {(dz, dx, array, way) for array in range(first, first + n)}


def schedule():
    rate, gap, latency = 46.7e3, 0.1, 2.0
    sends, waiting = [], forwards()
    free, coming, here, order = [0.0] * 3, [], set(), []

    def issue(now, send):
        link, _, _, _, n, rows = send
        free[link] = max(free[link], now) + n * rows[1] * WIDTH * 2 / rate + gap
        heapq.heappush(coming, (free[link] + latency, len(sends)))
        sends.append(send)

    for array in range(4):
        for send in own_sends(array):
            issue(0.0, send)
    for send in own_rest():
        issue(0.0, send)
    while coming:
        now, number = heapq.heappop(coming)
        link, dz, dx, first, n, rows = sends[number]
        here |= cover(*seen_by_receiver(dz, dx, link), first, n, rows)
        ready = [send for send in waiting if cover(*send[1:]) <= here]
        waiting = [send for send in waiting if send not in ready]
        for send in ready:
            issue(now, send)
        order.append((now, number, len(ready)))
    assert not waiting
    return sends, order


def merge(weight, left, right):
    product = lax.dot_general(left, right, (((0,), (0,)), ((), ())), preferred_element_type=jnp.float32)
    return (weight.astype(jnp.float32) + mix_rate * product).astype(jnp.bfloat16)


def gather_kernel(
    cols,
    weight_query, low_query, high_query,
    weight_key, low_key, high_key,
    weight_value, low_value, high_value,
    weight_mixed, low_mixed, high_mixed,
    norm_train, norm_step,
    stack, mixed, norm_slots,
    weights, lefts, rights, mixed_pair, norms, norm_parts,
    in_sem, link_send, link_recv, core_send, core_recv, pair_sem, norm_send, norm_recv,
):
    f, c = lax.axis_index("fsdp"), lax.axis_index("cols")
    z, x, core = lax.div(f, X * CORES), lax.rem(lax.div(f, CORES), X), lax.rem(f, CORES)
    chip = lax.div(f, CORES)

    def at(device_z, device_x, device_core):
        return {"fsdp": device_z * (X * CORES) + device_x * CORES + device_core}

    neighbour = {
        RIGHT: at(lax.rem(z + 1, Z), x, core),
        LEFT: at(lax.rem(z + Z - 1, Z), x, core),
        ACROSS: at(z, 1 - x, core),
    }
    twin = at(z, x, 1 - core)
    up, down = {"cols": lax.rem(c + 2, cols)}, {"cols": lax.rem(c + cols - 2, cols)}
    over = {"cols": c + 1 - 2 * lax.rem(c, 2)}

    barrier = pltpu.get_barrier_semaphore()
    others = [(dz, dx) for dz in range(Z) for dx in range(X) if (dz, dx) != (0, 0)]
    others_at = [at(lax.rem(z + dz, Z), lax.rem(x + dx, X), core) for dz, dx in others]
    peers = [*others_at, twin, up, down, over]
    for peer in peers:
        pl.semaphore_signal(barrier, inc=1, device_id=peer, device_id_type=pl.DeviceIdType.MESH)

    inputs = (
        (weight_query, low_query, high_query),
        (weight_key, low_key, high_key),
        (weight_value, low_value, high_value),
        (weight_mixed, high_mixed, low_mixed),
    )
    loads = {}
    for k in (QUERY, KEY, MIXED, VALUE):
        targets = (weights.at[k], lefts.at[k], rights.at[k])
        loads[k] = [
            pltpu.make_async_copy(source, target, in_sem.at[3 * k + n])
            for n, (source, target) in enumerate(zip(inputs[k], targets))
        ]
    loads[4] = [
        pltpu.make_async_copy(source, norms.at[n], in_sem.at[12 + n]) for n, source in enumerate((norm_train, norm_step))
    ]
    for copies in loads.values():
        for copy in copies:
            copy.start()

    own_rows = pl.ds(pl.multiple_of(f * ROWS, 16), ROWS)
    own_half = pl.ds(pl.multiple_of(core * ROWS, 16), ROWS)

    def wait_loads(k):
        for copy in loads[k]:
            copy.wait()

    def merge_own(k):
        wait_loads(k)
        merged = merge(weights[k], lefts[k], rights[k])
        if k == MIXED:
            mixed_pair[own_half, :] = merged
        else:
            stack[k, own_rows, :] = merged

    started = []

    def remote(source, target, send_sem, recv_sem, device):
        copy = pltpu.make_async_remote_copy(
            src_ref=source,
            dst_ref=target,
            send_sem=send_sem,
            recv_sem=recv_sem,
            device_id=device,
            device_id_type=pl.DeviceIdType.MESH,
        )
        copy.start()
        started.append(copy)

    def view(dz, dx, device_core, first, n, rows):
        block = lax.rem(z + dz, Z) * X + lax.rem(x + dx, X)
        start, many = rows
        if first == MIXED:
            start = pl.multiple_of(device_core * ROWS + start, 16)
            return mixed.at[pl.ds(start, many), pl.ds(pl.multiple_of(block * WIDTH, 128), WIDTH)]
        start = pl.multiple_of((block * CORES + device_core) * ROWS + start, 16)
        return stack.at[pl.ds(first, n), pl.ds(start, many), :]

    sends, order = schedule()
    issued = []

    def send_next():
        number = len(issued)
        link, *what = sends[number]
        issued.append(number)
        block = view(what[0], what[1], core, *what[2:])
        remote(block, block, link_send.at[number], link_recv.at[number], neighbour[link])

    def hand_over(number, *what):
        block = view(what[0], what[1], core, *what[2:])
        remote(block, block, core_send.at[number], core_recv.at[number], twin)

    def landed(sem, number, device_core, *what):
        block = view(what[0], what[1], device_core, *what[2:])
        pltpu.make_async_copy(block, block, sem.at[number]).wait()

    def norm_copy(number, source, target, device):
        remote(source, target, norm_send.at[number], norm_recv.at[number], device)

    def norm_wait(number, buffer):
        pltpu.make_async_copy(buffer, buffer, norm_recv.at[number]).wait()

    mine, twins, chips_sum, below, above, beyond, line_sum, overs = (norm_parts.at[k] for k in range(8))

    def norm_start():
        wait_loads(4)
        piece = norms.shape[-1]
        gain = (norms[0] + norms[1]).astype(jnp.bfloat16)
        gain = jnp.broadcast_to(gain.astype(jnp.float32), (8, piece)).astype(jnp.bfloat16)
        offset = (core * cols + c) * piece
        lane = lax.broadcasted_iota(jnp.int32, (piece, 128), 1)
        element = lax.broadcasted_iota(jnp.int32, (piece, 128), 0)
        row = lax.broadcasted_iota(jnp.int32, (8, 128), 0)
        tile = jnp.zeros((8, 128), jnp.float32)
        for r in range(5):
            hot = jnp.where(lane + 128 * r == element + offset, 1.0, 0.0).astype(jnp.bfloat16)
            spread = jnp.dot(gain, hot, preferred_element_type=jnp.float32)
            tile = jnp.where(row == r, spread, tile)
        mine[chip] = tile

    def norm_to_group():
        for (dz, dx), device in zip(others, others_at):
            norm_copy((-dz % Z) * X + dx, mine.at[chip], mine.at[chip], device)

    def norm_to_twin():
        for dz, dx in others:
            there = lax.rem(z + dz, Z) * X + lax.rem(x + dx, X)
            norm_wait(dz * X + dx, mine.at[there])
        norm_copy(8, mine, twins, twin)

    def norm_add_twin():
        norm_wait(8, twins)
        chips_sum[...] = mine[...] + twins[...]

    def norm_to_line():
        norm_copy(9, chips_sum, below, up)
        norm_copy(10, chips_sum, above, down)

    def norm_along_line():
        norm_wait(9, below)
        norm_copy(11, below, beyond, up)
        norm_wait(10, above)

    def norm_add_line():
        norm_wait(11, beyond)
        line_sum[...] = chips_sum[...] + below[...] + above[...] + beyond[...]

    def norm_over():
        norm_copy(12, line_sum, overs, over)

    def norm_end():
        norm_wait(12, overs)
        norm_slots[...] = line_sum[...] + overs[...]

    norm_steps = [
        (16, norm_to_twin), (21, norm_add_twin), (24, norm_to_line), (30, norm_along_line),
        (36, norm_add_line), (39, norm_over), (76, norm_end),
    ]

    own = [(len(sends), 0, 0, QUERY, 2, (0, ROWS)), (len(sends) + 1, 0, 0, VALUE, 1, (0, ROWS))]
    merge_own(QUERY)
    merge_own(KEY)
    pl.semaphore_wait(barrier, len(peers))
    for _ in own_sends(QUERY):
        send_next()
    norm_start()
    merge_own(MIXED)
    norm_to_group()
    for _ in own_sends(KEY):
        send_next()
    merge_own(VALUE)
    half = mixed_pair.at[own_half, :]
    remote(half, half, pair_sem.at[0], pair_sem.at[1], twin)
    pair = started[-1]
    hand_over(*own[0])

    pair.wait_recv()
    turned = mixed_pair[...].astype(jnp.float32).T.astype(jnp.bfloat16)
    mixed[:, pl.ds(pl.multiple_of(chip * WIDTH, 128), WIDTH)] = turned
    for _ in own_sends(VALUE):
        send_next()
    hand_over(*own[1])
    for _ in own_sends(MIXED) + own_rest():
        send_next()

    for now, number, ready in order:
        link, dz, dx, *what = sends[number]
        dz, dx = seen_by_receiver(dz, dx, link)
        landed(link_recv, number, core, dz, dx, *what)
        for _ in range(ready):
            send_next()
        hand_over(number, dz, dx, *what)
        if norm_steps and now >= norm_steps[0][0]:
            norm_steps.pop(0)[1]()
    assert not norm_steps

    for number, dz, dx, *what in own:
        landed(core_recv, number, 1 - core, dz, dx, *what)
    for _, number, _ in order:
        link, dz, dx, *what = sends[number]
        dz, dx = seen_by_receiver(dz, dx, link)
        landed(core_recv, number, 1 - core, dz, dx, *what)
    for copy in started:
        copy.wait_send()


def store_kernel(stack, mixed, slots, out_query, out_key, out_value, out_mixed, out_norm, gains, sems):
    copies = []

    def store(source, target):
        copy = pltpu.make_async_copy(source, target, sems.at[len(copies)])
        copy.start()
        copies.append(copy)

    for k, target in enumerate((out_query, out_key, out_value)):
        for part in range(4):
            rows = pl.ds(part * (FULL // 4), FULL // 4)
            store(stack.at[k, rows, :], target.at[rows, :])
    for part in range(4):
        rows = pl.ds(part * (WIDTH // 4), WIDTH // 4)
        store(mixed.at[rows, :], out_mixed.at[rows, :])
    tiles = [slots[chip][:5] for chip in range(CHIPS)]
    gains[...] = jnp.concatenate(tiles, axis=0).astype(jnp.bfloat16)
    store(gains, out_norm)
    for copy in copies:
        copy.wait()


def per_device(
    cols,
    weight_query, low_query, high_query,
    weight_key, low_key, high_key,
    weight_value, low_value, high_value,
    weight_mixed, low_mixed, high_mixed,
    norm_train, norm_step,
):
    tall, wide = (FULL, WIDTH), (WIDTH, FULL)
    piece = norm_train.shape[0]
    anywhere = pl.BlockSpec(memory_space=pl.ANY)
    in_vmem = pl.BlockSpec(memory_space=pltpu.VMEM)
    n_link = len(schedule()[0])
    gathered = pl.pallas_call(
        functools.partial(gather_kernel, cols),
        name="gather",
        out_shape=[
            pltpu.VMEM((3, *tall), jnp.bfloat16),
            pltpu.VMEM(wide, jnp.bfloat16),
            pltpu.VMEM((CHIPS, 8, 128), jnp.float32),
        ],
        in_specs=[pl.BlockSpec(memory_space=pltpu.HBM)] * 14,
        out_specs=[in_vmem] * 3,
        scratch_shapes=[
            pltpu.VMEM((4, ROWS, WIDTH), jnp.bfloat16),
            pltpu.VMEM((4, RANK, ROWS), jnp.bfloat16),
            pltpu.VMEM((4, RANK, WIDTH), jnp.bfloat16),
            pltpu.VMEM((WIDTH, WIDTH), jnp.bfloat16),
            pltpu.VMEM((2, 1, piece), jnp.float32),
            pltpu.VMEM((8, CHIPS, 8, 128), jnp.float32),
            pltpu.SemaphoreType.DMA((14,)),
            pltpu.SemaphoreType.DMA((n_link,)),
            pltpu.SemaphoreType.DMA((n_link,)),
            pltpu.SemaphoreType.DMA((n_link + 2,)),
            pltpu.SemaphoreType.DMA((n_link + 2,)),
            pltpu.SemaphoreType.DMA((2,)),
            pltpu.SemaphoreType.DMA((13,)),
            pltpu.SemaphoreType.DMA((13,)),
        ],
        compiler_params=pltpu.CompilerParams(
            collective_id=0, has_side_effects=True, vmem_limit_bytes=40_690_000
        ),
    )(
        weight_query, low_query.T, high_query,
        weight_key, low_key.T, high_key,
        weight_value, low_value.T, high_value,
        weight_mixed.T, low_mixed.T, high_mixed,
        norm_train.reshape(1, piece), norm_step.reshape(1, piece),
    )
    *ready, gains = pl.pallas_call(
        store_kernel,
        name="store",
        out_shape=[jax.ShapeDtypeStruct(tall, jnp.bfloat16)] * 3
        + [jax.ShapeDtypeStruct(wide, jnp.bfloat16), jax.ShapeDtypeStruct((CHIPS * 5, 128), jnp.bfloat16)],
        in_specs=[in_vmem] * 3,
        out_specs=[anywhere] * 5,
        scratch_shapes=[pltpu.VMEM((CHIPS * 5, 128), jnp.bfloat16), pltpu.SemaphoreType.DMA((17,))],
        compiler_params=pltpu.CompilerParams(vmem_limit_bytes=4 * 2**20),
    )(*gathered)
    return (*ready, gains.reshape(-1))


def solution(mesh):
    in_specs = (
        P("fsdp", "cols"),
        P("fsdp", None),
        P(None, "cols"),
        P("fsdp", "cols"),
        P("fsdp", None),
        P(None, "cols"),
        P("fsdp", "cols"),
        P("fsdp", None),
        P(None, "cols"),
        P("cols", "fsdp"),
        P("cols", None),
        P(None, "fsdp"),
        P(("fsdp", "cols")),
        P(("fsdp", "cols")),
    )
    out_specs = (P(None, "cols"), P(None, "cols"), P(None, "cols"), P("cols", None), P())
    return jax.shard_map(
        functools.partial(per_device, mesh.shape["cols"]),
        mesh=mesh,
        in_specs=in_specs,
        out_specs=out_specs,
        check_vma=False,
    )
```
